32 devices in a mesh: rep: 2 (over y), pipe: 2 (over core), tp: 8 (over z, x).
Axes of the slice: x: 2, y: 2, z: 4, core: 2. Of those that a mesh axis runs over, the one named last changes fastest.
Arguments:
- hidden_entering: bfloat16 [2, 120, 8192], P('rep', None, 'tp'), parts along dimension 0, may hold values from -60 to 60
- segment_adapter: int32 [2, 3], P('rep'), parts along dimension 0, may hold values from 0 to 127, as said below
- segment_requests: int32 [2, 3], P('rep'), parts along dimension 0, may hold values from 10 to 40, as said below
- section_norm_gain: float32 [2, 8192], P('pipe'), may hold values from 0.25 to 1.75
- up_matrix: bfloat16 [2, 14336, 8192], P('pipe', 'tp'), may hold values from -0.0625 to 0.0625
- down_matrix: bfloat16 [2, 8192, 14336], P('pipe', 'tp'), may hold values from -0.046875 to 0.046875
- adapter_reduce: bfloat16 [2, 128, 131072], P('pipe', None, 'tp'), may hold values from -0.0625 to 0.0625
- adapter_expand: bfloat16 [2, 128, 229376], P('pipe', None, 'tp'), may hold values from -1.5 to 1.5
Outputs:
- section_out: bfloat16 [2, 2, 120, 8192], P('pipe', 'rep', None, 'tp'), parts along dimension 1
The draws below stay inside these ranges and needn't reach their ends.
There are 2 independent parts, one for each index of `rep`. The reference program is written for one: setup_inputs(seed, part) draws one part's arguments, and reference() takes and returns one part's arrays. A program takes and returns all parts, laid end to end along the dimension named above; an argument that names none is the same for every part. Nothing has to cross between parts.
Inputs may be any that keep to these rules, and one draw needn't show every extreme that they name: `segment_adapter`: within each micro-batch the adapter ids of its segments do not decrease. The first segment_requests[m, j] rows of segment j of micro-batch m hold requests; the other rows are padding.
All inputs are finite; a program needn't handle non-finite values.
Results may differ from the reference program's by a relative error of at most 0.0045.
Values may be sent and summed in bfloat16 or wider, within the bound.
No kernel may reach another device: no remote copies, remote signals or barrier semaphores. Data moves between devices by JAX's collectives and lax.ppermute only.
A program may use at most 128 MiB of HBM per device.

```python
import math
import jax
import jax.numpy as jnp
from jax import lax

MODEL_DIMENSION = 8192
FEEDFORWARD_UNITS = 14336
ADAPTER_RANK = 16
ADAPTER_COUNT = 128
SEG = 40
SPM = 3
MB = 1
N_PIPE = 2


def draw_hidden_entering(key, part):
    row_count = SPM * SEG
    keys = jax.random.split(jax.random.fold_in(key, 101), 3)
    row_scale = jnp.exp(jax.random.uniform(keys[0], (MB, row_count, 1), jnp.float32, math.log(0.4), math.log(4.0)))
    rising = jnp.exp(math.log(3.0) * jnp.arange(MODEL_DIMENSION, dtype=jnp.float32) / MODEL_DIMENSION)
    col_scale = jnp.exp(jax.random.uniform(keys[1], (MODEL_DIMENSION,), jnp.float32, math.log(0.4), math.log(4.0))) * rising / 1.7
    values = jax.random.normal(keys[2], (MB, row_count, MODEL_DIMENSION), jnp.float32)
    return jnp.clip(values * row_scale * col_scale, -60.0, 60.0).astype(jnp.bfloat16)


def draw_segment_adapter(key, part):
    raw = jax.random.randint(jax.random.fold_in(key, 7), (MB, SPM), 0, ADAPTER_COUNT)
    return jnp.sort(raw, axis=-1).astype(jnp.int32)


def draw_segment_requests(key, part):
    keys = jax.random.split(jax.random.fold_in(key, 13), 2)
    counts = jax.random.randint(keys[0], (MB * SPM,), SEG // 4, SEG + 1)
    chosen = jax.random.randint(keys[1], (), 0, MB * SPM)
    counts = jnp.where(jnp.arange(MB * SPM) == chosen, SEG, counts)
    return counts.reshape(MB, SPM).astype(jnp.int32)


def level_of(key, dims, cuts, least, largest):
    def one(position, shards_of):
        steps = jax.random.uniform(jax.random.fold_in(jax.random.fold_in(key, 6), position), (shards_of,), jnp.float32, least / len(cuts), largest / len(cuts))
        return jnp.repeat(jnp.exp(steps), dims[position] // shards_of).reshape((-1,) + (1,) * (len(dims) - position - 1))

    factor_of = one(*cuts[0])
    for cut in cuts[1:]:
        factor_of = factor_of * one(*cut)
    return factor_of


def bell_draw(key, extent, spread, most, shards=(), kind=jnp.bfloat16):
    loudness = level_of(key, extent, shards, -0.22, 0.18) if shards else 1.0
    entries = jax.random.normal(key, extent, jnp.float32) * spread * loudness
    return jnp.minimum(jnp.maximum(entries, -most), most).astype(kind)


def setup_inputs(seed: int = 0, part: int = 0) -> dict:
    seeds = jax.random.split(jax.random.key(seed), 9)
    part_keys = jax.random.split(jax.random.fold_in(seeds[8], part), 9)
    hidden_entering = draw_hidden_entering(jax.random.fold_in(jax.random.fold_in(seeds[8], part), 71), part)
    segment_adapter = draw_segment_adapter(jax.random.fold_in(jax.random.fold_in(seeds[8], part), 71), part)
    segment_requests = draw_segment_requests(jax.random.fold_in(jax.random.fold_in(seeds[8], part), 71), part)
    section_norm_gain = jnp.clip(1.0 + 0.15 * jax.random.normal(seeds[3], (N_PIPE, MODEL_DIMENSION), jnp.float32), 0.25, 1.75)
    up_matrix = bell_draw(seeds[4], (N_PIPE, FEEDFORWARD_UNITS, MODEL_DIMENSION), MODEL_DIMENSION ** -0.5, 0.0625, ((0, 2), (1, 8)))
    down_matrix = bell_draw(seeds[5], (N_PIPE, MODEL_DIMENSION, FEEDFORWARD_UNITS), FEEDFORWARD_UNITS ** -0.5, 0.046875, ((0, 2), (1, 8)))
    adapter_reduce = bell_draw(seeds[6], (N_PIPE, ADAPTER_COUNT, MODEL_DIMENSION * ADAPTER_RANK), MODEL_DIMENSION ** -0.5, 0.0625, ((0, 2), (2, 8)))
    adapter_expand = bell_draw(seeds[7], (N_PIPE, ADAPTER_COUNT, FEEDFORWARD_UNITS * ADAPTER_RANK), ADAPTER_RANK ** -0.5, 1.5, ((0, 2), (2, 8)))
    return dict(hidden_entering=hidden_entering, segment_adapter=segment_adapter, segment_requests=segment_requests, section_norm_gain=section_norm_gain, up_matrix=up_matrix, down_matrix=down_matrix, adapter_reduce=adapter_reduce, adapter_expand=adapter_expand)


EPSILON = 1e-05

def times_rows(left, weight):
    return lax.dot_general(left, weight, (((1,), (1,)), ((), ())), preferred_element_type=jnp.float32)

def apply_section(hidden_flow, section_ordinal, segment_adapter, segment_requests, section_norm_gain, up_matrix, down_matrix, adapter_reduce, adapter_expand):
    batch_list = hidden_flow.shape[0]
    row_count = hidden_flow.shape[1]
    feature_width = hidden_flow.shape[2]
    hidden_extent = up_matrix.shape[1]
    batch_results = segment_adapter.shape[1]
    seg_rows = row_count // batch_results
    adapter_rank_count = adapter_reduce.shape[2] // feature_width
    widened = hidden_flow.astype(jnp.float32)
    scaled = (widened * section_norm_gain[section_ordinal]).astype(jnp.bfloat16)
    inverse = lax.rsqrt(lax.optimization_barrier(jnp.mean(widened * widened, axis=-1, keepdims=True)) + EPSILON)
    flat_scaled = scaled.reshape(batch_list * row_count, feature_width)
    base_up = times_rows(flat_scaled, up_matrix[section_ordinal]).reshape(batch_list, row_count, hidden_extent)
    input_panel = adapter_reduce[section_ordinal][segment_adapter].reshape(batch_list, batch_results, feature_width, adapter_rank_count).astype(jnp.float32)
    output_panel = adapter_expand[section_ordinal][segment_adapter].reshape(batch_list, batch_results, hidden_extent, adapter_rank_count).astype(jnp.float32)
    segment_scaled = scaled.reshape(batch_list, batch_results, seg_rows, feature_width).astype(jnp.float32)
    shrunk = jnp.einsum('msdr,mspd->msrp', input_panel, segment_scaled)
    low_rank = (inverse.reshape(batch_list, batch_results, 1, seg_rows) * shrunk).astype(jnp.bfloat16)
    adapted = jnp.einsum('msrp,msdr->mspd', low_rank.astype(jnp.float32), output_panel).reshape(batch_list, row_count, hidden_extent)
    up_sum = inverse * base_up + adapted
    hidden_act = jax.nn.silu(up_sum).astype(jnp.bfloat16)
    down_sum = times_rows(hidden_act.reshape(batch_list * row_count, hidden_extent), down_matrix[section_ordinal]).reshape(batch_list, row_count, feature_width)
    updated = (widened + down_sum).astype(jnp.bfloat16)
    positions = lax.broadcasted_iota(jnp.int32, (batch_list, batch_results, seg_rows), 2)
    row_kept = (positions < segment_requests[:, :, None]).reshape(batch_list, row_count, 1)
    return jnp.where(row_kept, updated, jnp.zeros_like(updated))

def reference(hidden_entering, segment_adapter, segment_requests, section_norm_gain, up_matrix, down_matrix, adapter_reduce, adapter_expand):
    hidden_flow = hidden_entering
    outputs = []
    for section_ordinal in range(N_PIPE):
        hidden_flow = apply_section(hidden_flow, section_ordinal, segment_adapter, segment_requests, section_norm_gain, up_matrix, down_matrix, adapter_reduce, adapter_expand)
        outputs.append(hidden_flow)
    return jnp.stack(outputs)
```

```python
import functools

import jax
import jax.numpy as jnp
from jax import lax
from jax.experimental import pallas as pl
from jax.experimental.pallas import tpu as pltpu
from jax.sharding import PartitionSpec as P

EPSILON = 1e-05
LANES = 128
VMEM_GRANT = 40 * 1024 * 1024


def shifted(x, axis, by):
    size = lax.axis_size(axis)
    pairs = [(i, i + by) for i in range(size) if 0 <= i + by < size]
    return lax.ppermute(x, axis, pairs)


def times_rows(left, weight):
    return lax.dot_general(
        left, weight, (((1,), (1,)), ((), ())), preferred_element_type=jnp.float32
    )


def block_step(
    current, unit_ids, unit_live, gain_full, up_weight, down_weight, shrink_weight, expand_weight
):
    row_count = current.shape[0]
    col_count = current.shape[1]
    hid_count = up_weight.shape[0]
    segments = unit_ids.shape[0]
    seg_rows = row_count // segments
    feature_width = gain_full.shape[0]
    adapter_rank_count = shrink_weight.shape[1] // col_count
    column = lax.axis_index("tp") * col_count
    gain_mine = lax.dynamic_slice_in_dim(gain_full, column, col_count, 0)
    widened_local = current.astype(jnp.float32)
    local_scaled = (widened_local * gain_mine).astype(jnp.bfloat16)
    input_panel = shrink_weight[unit_ids].reshape(segments, col_count, adapter_rank_count)
    output_panel = expand_weight[unit_ids].reshape(segments, hid_count, adapter_rank_count)
    partial_value = jnp.einsum(
        "sdr,spd->rsp",
        input_panel,
        local_scaled.reshape(segments, seg_rows, col_count),
        preferred_element_type=jnp.float32,
    ).reshape(adapter_rank_count, row_count)
    local_squares = jnp.sum(widened_local * widened_local, axis=1)
    reduced, squares = lax.psum((partial_value, local_squares), "tp")
    widened = lax.all_gather(current, "tp", axis=1, tiled=True).astype(jnp.float32)
    scaled = (widened * gain_full).astype(jnp.bfloat16)
    up_total = times_rows(scaled, up_weight)
    inverse = lax.rsqrt(squares / feature_width + EPSILON)
    low_rank = (
        (reduced * inverse[None, :])
        .astype(jnp.bfloat16)
        .reshape(adapter_rank_count, segments, seg_rows)
    )
    adapted = jnp.einsum(
        "rsp,sdr->spd", low_rank, output_panel, preferred_element_type=jnp.float32
    ).reshape(row_count, hid_count)
    up_sum = inverse[:, None] * up_total + adapted
    hidden_act = jax.nn.silu(up_sum).astype(jnp.bfloat16)
    down_sum = times_rows(lax.all_gather(hidden_act, "tp", axis=1, tiled=True), down_weight)
    updated = (widened_local + down_sum).astype(jnp.bfloat16)
    positions = lax.broadcasted_iota(jnp.int32, (segments, seg_rows), 1)
    row_kept = (positions < unit_live[:, None]).reshape(row_count, 1)
    return jnp.where(row_kept, updated, jnp.zeros_like(updated))


def run_window(
    units, unit_ids, unit_live, gain_full, up_weight, down_weight, shrink_weight, expand_weight
):
    section_index = lax.axis_index("pipe")
    sections = lax.axis_size("pipe")
    unit_count = units.shape[0]
    tick_total = unit_count + sections - 1

    def process(tick_index, received, collected):
        position = jnp.clip(tick_index - section_index, 0, unit_count - 1)
        arriving = lax.dynamic_index_in_dim(
            units, jnp.minimum(tick_index, unit_count - 1), 0, keepdims=False
        )
        current = jnp.where(section_index == 0, arriving, received)
        ids_here = lax.dynamic_index_in_dim(unit_ids, position, 0, keepdims=False)
        live_here = lax.dynamic_index_in_dim(unit_live, position, 0, keepdims=False)
        produced = block_step(
            current,
            ids_here,
            live_here,
            gain_full,
            up_weight,
            down_weight,
            shrink_weight,
            expand_weight,
        )
        lag = tick_index - section_index
        in_window = jnp.logical_and(lag >= 0, lag < unit_count)
        placed = lax.dynamic_update_index_in_dim(collected, produced, position, 0)
        return (produced, jnp.where(in_window, placed, collected))

    def one_tick(tick_index, state):
        produced, collected = process(tick_index, state[0], state[1])
        return (shifted(produced, "pipe", 1), collected)

    start_state = (jnp.zeros_like(units[0]), jnp.zeros_like(units))
    received, collected = lax.fori_loop(0, tick_total - 1, one_tick, start_state)
    produced, collected = process(tick_total - 1, received, collected)
    return collected


def vmem():
    return pl.BlockSpec(memory_space=pltpu.VMEM)


def smem():
    return pl.BlockSpec(memory_space=pltpu.SMEM)


def kernel_call(body, outs, flops, moved, name, aliases=None, scratch=()):
    return dict(
        kernel=body,
        out_shape=outs,
        input_output_aliases=aliases or {},
        scratch_shapes=list(scratch),
        compiler_params=pltpu.CompilerParams(vmem_limit_bytes=VMEM_GRANT),
        cost_estimate=pl.CostEstimate(flops=flops, bytes_accessed=moved, transcendentals=0),
        name=name,
    )


def write_payload(out_ref, rows, panel, seg_rows, rank):
    row_count, cols = rows.shape
    width = panel.shape[0]
    both = lax.dot_general(
        rows, panel, (((1,), (1,)), ((), ())), preferred_element_type=jnp.float32
    )
    owner = lax.broadcasted_iota(jnp.int32, (row_count, rank), 0)
    part = jnp.zeros((row_count, rank), jnp.float32)
    for s in range(width // rank):
        inside = jnp.logical_and(owner >= s * seg_rows, owner < (s + 1) * seg_rows)
        part = part + jnp.where(inside, both[:, s * rank : (s + 1) * rank], 0.0)
    high = part.astype(jnp.bfloat16)
    low = (part - high.astype(jnp.float32)).astype(jnp.bfloat16)
    out_ref[:, :cols] = rows
    out_ref[:, cols:] = jnp.concatenate(
        [high, low, jnp.zeros((row_count, LANES - 2 * rank), jnp.bfloat16)], axis=1
    )


def payload_body(x_ref, panel_ref, out_ref, *, seg_rows, rank):
    write_payload(out_ref, x_ref[...], panel_ref[...], seg_rows, rank)


def make_payload(x, panel, seg_rows, rank):
    rows, cols = x.shape
    out = jax.ShapeDtypeStruct((rows, cols + LANES), jnp.bfloat16)
    spec = kernel_call(
        functools.partial(payload_body, seg_rows=seg_rows, rank=rank),
        out,
        2 * rows * cols * panel.shape[0],
        4 * rows * cols,
        "payload",
    )
    return pl.pallas_call(in_specs=[vmem(), vmem()], out_specs=vmem(), **spec)(x, panel)


def stream(weight, buffer, sems, plan, slots):
    def copy(i):
        return pltpu.make_async_copy(
            weight.at[plan[i][0], plan[i][1]], buffer.at[i % slots], sems.at[i % slots]
        )

    return copy


def up_body(
    info_ref, *refs, count, begin, finish, tile, slots, cols, seg_rows, rank, features, row_count
):
    payloads = refs[:count]
    refs = refs[count:]
    gain_ref, weight_ref = refs[:2]
    refs = refs[2:]
    if finish:
        panel_ref, refs = refs[0], refs[1:]
    if not begin:
        refs = refs[2:]
    if finish:
        act_ref, total_ref, stat_ref, buffer, sems = refs
    else:
        total_ref, stat_ref, buffer, sems = refs
    units = weight_ref.shape[0]
    tiles = units // tile

    @pl.when(info_ref[0] == 1)
    def _():
        plan = []
        for c in range(count):
            start = pl.multiple_of(info_ref[1 + c] * cols, cols)
            for j in range(tiles):
                plan.append((pl.ds(j * tile, tile), pl.ds(start, cols), c, j))
        copy = stream(weight_ref, buffer, sems, plan, slots)
        for i in range(min(slots, len(plan))):
            copy(i).start()
        scaled = []
        for c in range(count):
            start = pl.multiple_of(info_ref[1 + c] * cols, cols)
            wide = payloads[c][:, :cols].astype(jnp.float32)
            scaled.append((wide * gain_ref[:, pl.ds(start, cols)]).astype(jnp.bfloat16))
            squares = jnp.sum(wide * wide, axis=1, keepdims=True)
            extra = payloads[c][:, cols:].astype(jnp.float32)
            low = extra[:, :rank] + extra[:, rank : 2 * rank]
            stat = jnp.concatenate(
                [low, jnp.broadcast_to(squares, (row_count, LANES - rank))], axis=1
            )
            if begin and c == 0:
                stat_ref[...] = stat
            else:
                stat_ref[...] += stat
        for i, (_, _, c, j) in enumerate(plan):
            copy(i).wait()
            part = lax.dot_general(
                scaled[c],
                buffer[i % slots],
                (((1,), (1,)), ((), ())),
                preferred_element_type=jnp.float32,
            )
            here = (slice(None), pl.ds(j * tile, tile))
            if begin and c == 0:
                total_ref[here] = part
            else:
                total_ref[here] += part
            if i + slots < len(plan):
                copy(i + slots).start()
        if finish:
            inverse = lax.rsqrt(stat_ref[:, rank : rank + 1] / features + EPSILON)
            low = (inverse * stat_ref[:, :rank]).astype(jnp.bfloat16)
            width = panel_ref.shape[0]
            tiled = jnp.concatenate([low] * (width // rank), axis=1).astype(jnp.float32)
            row = lax.broadcasted_iota(jnp.int32, (row_count, width), 0)
            col = lax.broadcasted_iota(jnp.int32, (row_count, width), 1)
            keep = jnp.zeros((row_count, width), jnp.bool_)
            for s in range(width // rank):
                mine = jnp.logical_and(row >= s * seg_rows, row < (s + 1) * seg_rows)
                here = jnp.logical_and(col >= s * rank, col < (s + 1) * rank)
                keep = jnp.logical_or(keep, jnp.logical_and(mine, here))
            spread = jnp.where(keep, tiled, 0.0).astype(jnp.bfloat16)
            for j in range(tiles):
                here = (slice(None), pl.ds(j * tile, tile))
                adapted = jnp.dot(
                    spread, panel_ref[:, pl.ds(j * tile, tile)], preferred_element_type=jnp.float32
                )
                value = inverse * total_ref[here] + adapted
                act_ref[here] = (value / (1.0 + jnp.exp(-value))).astype(jnp.bfloat16)


def split_tile(size, parts):
    tile = size // parts
    return tile if tile * parts == size and tile % LANES == 0 else size


def up_call(state, payloads, indices, gate, gain, weight, panel, seg_rows, rank, features, tag):
    count = len(payloads)
    row_count = payloads[0].shape[0]
    cols = payloads[0].shape[1] - LANES
    units = weight.shape[0]
    begin = state is None
    finish = panel is not None
    tile = split_tile(units, 2)
    slots = min(4, count * (units // tile))
    info = jnp.stack([gate] + indices).astype(jnp.int32)
    operands = [info] + payloads + [gain, weight]
    specs = [smem()] + [vmem()] * (count + 1) + [pl.BlockSpec(memory_space=pl.ANY)]
    if finish:
        operands.append(panel)
        specs.append(vmem())
    outs = [
        jax.ShapeDtypeStruct((row_count, units), jnp.float32),
        jax.ShapeDtypeStruct((row_count, LANES), jnp.float32),
    ]
    if finish:
        outs = [jax.ShapeDtypeStruct((row_count, units), jnp.bfloat16)] + outs
    aliases = {}
    if not begin:
        for k in range(2):
            aliases[len(operands)] = k + int(finish)
            operands.append(state[k])
            specs.append(vmem())
    spec = kernel_call(
        functools.partial(
            up_body,
            count=count,
            begin=begin,
            finish=finish,
            tile=tile,
            slots=slots,
            cols=cols,
            seg_rows=seg_rows,
            rank=rank,
            features=features,
            row_count=row_count,
        ),
        tuple(outs),
        2 * row_count * units * cols * count,
        2 * units * cols * count,
        "up_" + tag,
        aliases,
        [pltpu.VMEM((slots, tile, cols), jnp.bfloat16), pltpu.SemaphoreType.DMA((slots,))],
    )
    return pl.pallas_call(in_specs=specs, out_specs=(vmem(),) * len(outs), **spec)(*operands)


def down_body(
    info_ref, *refs, count, begin, finish, tile, slots, units, seg_rows, rank, row_count, segments
):
    acts = refs[:count]
    refs = refs[count:]
    weight_ref, refs = refs[0], refs[1:]
    if finish:
        own_ref, refs = refs[0], refs[1:]
    if finish == "next":
        panel_ref, refs = refs[0], refs[1:]
    if finish == "last":
        earlier_ref, refs = refs[0], refs[1:]
    if not begin:
        total_in, refs = refs[0], refs[1:]
    if finish:
        out_ref, refs = refs[0], refs[1:]
    if finish and not begin:
        buffer, sems = refs
        total_ref = total_in
    else:
        total_ref, buffer, sems = refs
    cols = weight_ref.shape[0]
    tiles = cols // tile

    @pl.when(info_ref[0] == 1)
    def _():
        plan = []
        for c in range(count):
            start = pl.multiple_of(info_ref[1 + c] * units, LANES)
            for j in range(tiles):
                plan.append((pl.ds(j * tile, tile), pl.ds(start, units), c, j))
        copy = stream(weight_ref, buffer, sems, plan, slots)
        for i in range(min(slots, len(plan))):
            copy(i).start()
        if finish:
            row = lax.broadcasted_iota(jnp.int32, (row_count, 1), 0)
            keep = jnp.zeros((row_count, 1), jnp.bool_)
            for s in range(segments):
                live = info_ref[1 + count + s] + s * seg_rows
                keep = jnp.logical_or(keep, jnp.logical_and(row >= s * seg_rows, row < live))
        parts = {}
        for i, (_, _, c, j) in enumerate(plan):
            copy(i).wait()
            part = lax.dot_general(
                acts[c][...],
                buffer[i % slots],
                (((1,), (1,)), ((), ())),
                preferred_element_type=jnp.float32,
            )
            here = (slice(None), pl.ds(j * tile, tile))
            if finish:
                parts[j] = part if c == 0 else parts[j] + part
                if c == count - 1:
                    value = own_ref[here].astype(jnp.float32) + (total_ref[here] + parts[j])
                    out_ref[here] = jnp.where(keep, value, 0.0).astype(jnp.bfloat16)
            elif begin and c == 0:
                total_ref[here] = part
            else:
                total_ref[here] += part
            if i + slots < len(plan):
                copy(i + slots).start()
        if finish == "next":
            write_payload(out_ref, out_ref[:, :cols], panel_ref[...], seg_rows, rank)

    if finish == "last":

        @pl.when(info_ref[0] == 0)
        def _():
            out_ref[...] = earlier_ref[:, :cols]


def down_call(total, acts, indices, gate, weight, seg_rows, rank, tag, live, own=None, panel=None,
              earlier=None):
    count = len(acts)
    row_count, units = acts[0].shape
    cols = weight.shape[0]
    begin = total is None
    finish = None if own is None else ("next" if panel is not None else "last")
    tile = split_tile(cols, 2)
    slots = min(4, count * (cols // tile))
    segments = live.shape[0]
    info = jnp.concatenate([jnp.stack([gate] + indices).astype(jnp.int32), live])
    operands = [info] + acts + [weight]
    specs = [smem()] + [vmem()] * count + [pl.BlockSpec(memory_space=pl.ANY)]
    for extra in (own, panel, earlier):
        if extra is not None:
            operands.append(extra)
            specs.append(vmem())
    aliases = {}
    if not begin:
        if not finish:
            aliases[len(operands)] = 0
        operands.append(total)
        specs.append(vmem())
    if finish == "next":
        out = jax.ShapeDtypeStruct((row_count, cols + LANES), jnp.bfloat16)
    elif finish == "last":
        out = jax.ShapeDtypeStruct((row_count, cols), jnp.bfloat16)
    else:
        out = jax.ShapeDtypeStruct((row_count, cols), jnp.float32)
    spec = kernel_call(
        functools.partial(
            down_body,
            count=count,
            begin=begin,
            finish=finish,
            tile=tile,
            slots=slots,
            units=units,
            seg_rows=seg_rows,
            rank=rank,
            row_count=row_count,
            segments=segments,
        ),
        out,
        2 * row_count * units * cols * count,
        2 * units * cols * count,
        "down_" + tag,
        aliases,
        [pltpu.VMEM((slots, tile, units), jnp.bfloat16), pltpu.SemaphoreType.DMA((slots,))],
    )
    return pl.pallas_call(in_specs=specs, out_specs=vmem(), **spec)(*operands)


def ladder(rails):
    size = lax.axis_size("tp")
    rungs = size // rails

    def pairs(source, target, move):
        out = []
        for t in range(size):
            rung, rail = divmod(t, rails)
            to_rung, to_rail = move(rung, rail)
            out.append((source * size + t, target * size + to_rung % rungs * rails + to_rail))
        return out

    def send(value, source, target, move):
        return lax.ppermute(value, ("pipe", "tp"), pairs(source, target, move))

    return rungs, send


def spread(value, helper, worker, rungs, rails, send):
    me = lax.axis_index("tp")
    rung, rail = me // rails, me % rails
    other = 1 - rail

    def owner(step, on):
        return (rung - step + rungs) % rungs * rails + on

    order = sorted(range(1, rungs), key=lambda k: min(k, rungs - k))
    direct = {
        k: send(value, helper, worker, lambda g, r, k=k: (g + k, r)) for k in order
    }
    across = send(value, helper, worker, lambda g, r: (g, 1 - r))
    found = [(across, owner(0, other))]
    for k in order:
        found.append((direct[k], owner(k, rail)))
        found.append((send(direct[k], worker, worker, lambda g, r: (g, 1 - r)), owner(k, other)))
    return found


def grouped(found):
    groups = [found[:2]]
    rest = found[2:]
    while len(rest) > 1:
        groups.append(rest[:2])
        rest = rest[2:]
    if rest:
        groups.append(rest)
    return groups


def run_ladder(
    rows, ids, live, gain, up_weight, down_weight, shrink_weight, expand_weight, rails
):
    row_count, cols = rows.shape
    segments = ids.shape[0]
    seg_rows = row_count // segments
    rank = shrink_weight.shape[1] // cols
    units = up_weight.shape[0]
    features = gain.shape[0]
    me = lax.axis_index("tp")
    stage = lax.axis_index("pipe")
    rungs, send = ladder(rails)

    def rows_of(table):
        return jnp.stack(
            [lax.dynamic_index_in_dim(table, ids[s], 0, keepdims=False) for s in range(segments)]
        )

    gain_mine = lax.dynamic_slice_in_dim(gain, me * cols, cols, 0)
    reduce_panel = rows_of(shrink_weight).reshape(segments, cols, rank)
    reduce_panel = (
        (reduce_panel.astype(jnp.float32) * gain_mine[None, :, None])
        .astype(jnp.bfloat16)
        .transpose(0, 2, 1)
        .reshape(segments * rank, cols)
    )
    expand_panel = (
        rows_of(expand_weight)
        .reshape(segments, units, rank)
        .transpose(0, 2, 1)
        .reshape(segments * rank, units)
    )
    size = lax.axis_size("tp")
    swap = [(i, (i + size) % (2 * size)) for i in range(2 * size)]
    partner_panel = lax.ppermute(reduce_panel, ("pipe", "tp"), swap)
    gain_row = gain.reshape(1, features)
    first_panel = jnp.where(stage == 0, reduce_panel, partner_panel)
    carried = make_payload(rows, first_panel, seg_rows, rank)
    own = carried
    for k in range(2):
        worker, helper = k, 1 - k
        gate = (stage == k).astype(jnp.int32)
        if k:
            own = send(carried, helper, worker, lambda g, r: (g, r))
        found = spread(carried, helper, worker, rungs, rails, send)
        state = up_call(None, [own], [me], gate, gain_row, up_weight, None, seg_rows, rank,
                        features, f"{k}_own")
        groups = grouped(found)
        for i, group in enumerate(groups):
            last = i == len(groups) - 1
            state = up_call(
                state,
                [g[0] for g in group],
                [g[1] for g in group],
                gate,
                gain_row,
                up_weight,
                expand_panel if last else None,
                seg_rows,
                rank,
                features,
                f"{k}_{i}",
            )
        act = state[0]
        handed = send(act, worker, helper, lambda g, r: (g, r))
        found = spread(handed, helper, worker, rungs, rails, send)
        total = down_call(None, [act], [me], gate, down_weight, seg_rows, rank, f"{k}_own", live)
        groups = grouped(found)
        for i, group in enumerate(groups):
            last = i == len(groups) - 1
            extra = {}
            if last:
                extra = dict(own=own)
                if k == 0:
                    extra["panel"] = partner_panel
                else:
                    extra["earlier"] = carried
            total = down_call(
                total,
                [g[0] for g in group],
                [g[1] for g in group],
                gate,
                down_weight,
                seg_rows,
                rank,
                f"{k}_{i}",
                live,
                **extra,
            )
        if k == 0:
            carried = total
    return total


def per_device(
    hidden_entering,
    segment_adapter,
    segment_requests,
    section_norm_gain,
    up_matrix,
    down_matrix,
    adapter_reduce,
    adapter_expand,
):
    batch_list = hidden_entering.shape[0]
    row_count = hidden_entering.shape[1]
    col_count = hidden_entering.shape[2]
    size = lax.axis_size("tp")
    rails = 2
    fits = (
        lax.axis_size("pipe") == 2
        and batch_list == 1
        and size % rails == 0
        and size // rails <= 4
        and col_count % LANES == 0
        and up_matrix.shape[1] % LANES == 0
    )
    if fits:
        out = run_ladder(
            hidden_entering[0],
            segment_adapter[0],
            segment_requests[0],
            section_norm_gain[0],
            up_matrix[0],
            down_matrix[0],
            adapter_reduce[0],
            adapter_expand[0],
            rails,
        )
        return out.reshape(1, batch_list, row_count, col_count)
    collected = run_window(
        hidden_entering,
        segment_adapter,
        segment_requests,
        section_norm_gain[0],
        up_matrix[0],
        down_matrix[0],
        adapter_reduce[0],
        adapter_expand[0],
    )
    return collected.reshape(1, batch_list, row_count, col_count)


def solution(mesh):
    return jax.shard_map(
        per_device,
        mesh=mesh,
        in_specs=(
            P("rep", None, "tp"),
            P("rep", None),
            P("rep", None),
            P("pipe", None),
            P("pipe", "tp", None),
            P("pipe", "tp", None),
            P("pipe", None, "tp"),
            P("pipe", None, "tp"),
        ),
        out_specs=P("pipe", "rep", None, "tp"),
        check_vma=False,
    )
```

```python
import functools

import jax
import jax.numpy as jnp
from jax import lax
from jax.experimental import pallas as pl
from jax.experimental.pallas import tpu as pltpu
from jax.sharding import PartitionSpec as P


EPSILON = 1e-05
LANES = 128
PIECES = 4
VMEM_GRANT = 14 * 1024 * 1024


def shifted(x, axis, by):
    size = lax.axis_size(axis)
    pairs = [(i, i + by) for i in range(size) if 0 <= i + by < size]
    return lax.ppermute(x, axis, pairs)


def times_rows(left, weight):
    return lax.dot_general(
        left, weight, (((1,), (1,)), ((), ())), preferred_element_type=jnp.float32
    )


def block_step(
    current, unit_ids, unit_live, gain_full, up_weight, down_weight, shrink_weight, expand_weight
):
    row_count = current.shape[0]
    col_count = current.shape[1]
    hid_count = up_weight.shape[0]
    segments = unit_ids.shape[0]
    seg_rows = row_count // segments
    feature_width = gain_full.shape[0]
    adapter_rank_count = shrink_weight.shape[1] // col_count
    column = lax.axis_index("tp") * col_count
    gain_mine = lax.dynamic_slice_in_dim(gain_full, column, col_count, 0)
    widened_local = current.astype(jnp.float32)
    local_scaled = (widened_local * gain_mine).astype(jnp.bfloat16)
    input_panel = shrink_weight[unit_ids].reshape(segments, col_count, adapter_rank_count)
    output_panel = expand_weight[unit_ids].reshape(segments, hid_count, adapter_rank_count)
    partial_value = jnp.einsum(
        "sdr,spd->rsp",
        input_panel,
        local_scaled.reshape(segments, seg_rows, col_count),
        preferred_element_type=jnp.float32,
    ).reshape(adapter_rank_count, row_count)
    local_squares = jnp.sum(widened_local * widened_local, axis=1)
    reduced, squares = lax.psum((partial_value, local_squares), "tp")
    widened = lax.all_gather(current, "tp", axis=1, tiled=True).astype(jnp.float32)
    scaled = (widened * gain_full).astype(jnp.bfloat16)
    up_total = times_rows(scaled, up_weight)
    inverse = lax.rsqrt(squares / feature_width + EPSILON)
    low_rank = (
        (reduced * inverse[None, :])
        .astype(jnp.bfloat16)
        .reshape(adapter_rank_count, segments, seg_rows)
    )
    adapted = jnp.einsum(
        "rsp,sdr->spd", low_rank, output_panel, preferred_element_type=jnp.float32
    ).reshape(row_count, hid_count)
    up_sum = inverse[:, None] * up_total + adapted
    hidden_act = jax.nn.silu(up_sum).astype(jnp.bfloat16)
    down_sum = times_rows(lax.all_gather(hidden_act, "tp", axis=1, tiled=True), down_weight)
    updated = (widened_local + down_sum).astype(jnp.bfloat16)
    positions = lax.broadcasted_iota(jnp.int32, (segments, seg_rows), 1)
    row_kept = (positions < unit_live[:, None]).reshape(row_count, 1)
    return jnp.where(row_kept, updated, jnp.zeros_like(updated))


def run_window(
    units, unit_ids, unit_live, gain_full, up_weight, down_weight, shrink_weight, expand_weight
):
    section_index = lax.axis_index("pipe")
    sections = lax.axis_size("pipe")
    unit_count = units.shape[0]
    tick_total = unit_count + sections - 1

    def process(tick_index, received, collected):
        position = jnp.clip(tick_index - section_index, 0, unit_count - 1)
        arriving = lax.dynamic_index_in_dim(
            units, jnp.minimum(tick_index, unit_count - 1), 0, keepdims=False
        )
        current = jnp.where(section_index == 0, arriving, received)
        ids_here = lax.dynamic_index_in_dim(unit_ids, position, 0, keepdims=False)
        live_here = lax.dynamic_index_in_dim(unit_live, position, 0, keepdims=False)
        produced = block_step(
            current,
            ids_here,
            live_here,
            gain_full,
            up_weight,
            down_weight,
            shrink_weight,
            expand_weight,
        )
        lag = tick_index - section_index
        in_window = jnp.logical_and(lag >= 0, lag < unit_count)
        placed = lax.dynamic_update_index_in_dim(collected, produced, position, 0)
        return (produced, jnp.where(in_window, placed, collected))

    def one_tick(tick_index, state):
        produced, collected = process(tick_index, state[0], state[1])
        return (shifted(produced, "pipe", 1), collected)

    start_state = (jnp.zeros_like(units[0]), jnp.zeros_like(units))
    received, collected = lax.fori_loop(0, tick_total - 1, one_tick, start_state)
    _, collected = process(tick_total - 1, received, collected)
    return collected


def vmem():
    return pl.BlockSpec(memory_space=pltpu.VMEM)


def smem():
    return pl.BlockSpec(memory_space=pltpu.SMEM)


def anywhere():
    return pl.BlockSpec(memory_space=pltpu.MemorySpace.HBM)


def in_hbm(x):
    return pltpu.with_memory_space_constraint(x, pltpu.MemorySpace.HBM)


def kernel_call(body, outs, flops, moved, name, aliases=None, scratch=()):
    return dict(
        kernel=body,
        out_shape=outs,
        input_output_aliases=aliases or {},
        scratch_shapes=list(scratch),
        compiler_params=pltpu.CompilerParams(vmem_limit_bytes=VMEM_GRANT),
        cost_estimate=pl.CostEstimate(flops=flops, bytes_accessed=moved, transcendentals=0),
        name=name,
    )


def fetch_body(info_ref, gain_ref, *refs, segments, id_at, own_at, cols, tables):
    table_refs = refs[:tables]
    outs = refs[tables : tables + tables * segments + 1]
    buffers = refs[tables + tables * segments + 1 : -1]
    sems = refs[-1]
    copies = []
    for t in range(tables):
        for s in range(segments):
            first = pl.multiple_of(info_ref[id_at + s] // 8 * 8, 8)
            copies.append(
                pltpu.make_async_copy(
                    table_refs[t].at[pl.ds(first, 8), :],
                    buffers[t].at[s],
                    sems.at[t * segments + s],
                )
            )
    for copy in copies:
        copy.start()
    start = pl.multiple_of(info_ref[own_at] * cols, cols)
    outs[-1][...] = gain_ref[:, pl.ds(start, cols)]
    for t in range(tables):
        for s in range(segments):
            copies[t * segments + s].wait()
            block = buffers[t][s].astype(jnp.float32)
            row = lax.broadcasted_iota(jnp.int32, block.shape, 0)
            mine = jnp.where(row == info_ref[id_at + s] % 8, block, 0.0)
            outs[t * segments + s][...] = jnp.sum(mine, axis=0, keepdims=True).astype(
                jnp.bfloat16
            )


def fetch_rows(info, gain, tables, segments, id_at, own_at, cols):
    outs = [
        jax.ShapeDtypeStruct((1, t.shape[1]), jnp.bfloat16) for t in tables for _ in range(segments)
    ] + [jax.ShapeDtypeStruct((1, cols), jnp.float32)]
    spec = kernel_call(
        functools.partial(
            fetch_body,
            segments=segments,
            id_at=id_at,
            own_at=own_at,
            cols=cols,
            tables=len(tables),
        ),
        tuple(outs),
        0,
        sum(16 * segments * t.shape[1] for t in tables),
        "fetch",
        scratch=[pltpu.VMEM((segments, 8, t.shape[1]), jnp.bfloat16) for t in tables]
        + [pltpu.SemaphoreType.DMA((len(tables) * segments,))],
    )
    got = pl.pallas_call(
        in_specs=[smem(), vmem()] + [anywhere()] * len(tables),
        out_specs=(vmem(),) * len(outs),
        **spec,
    )(info, gain, *[in_hbm(t) for t in tables])
    rows = [got[t * segments : (t + 1) * segments] for t in range(len(tables))]
    return rows, got[-1]


def write_payload(out_ref, rows, panel, seg_rows, rank):
    row_count, cols = rows.shape
    width = panel.shape[0]
    both = lax.dot_general(
        rows, panel, (((1,), (1,)), ((), ())), preferred_element_type=jnp.float32
    )
    owner = lax.broadcasted_iota(jnp.int32, (row_count, rank), 0)
    part = jnp.zeros((row_count, rank), jnp.float32)
    for s in range(width // rank):
        inside = jnp.logical_and(owner >= s * seg_rows, owner < (s + 1) * seg_rows)
        part = part + jnp.where(inside, both[:, s * rank : (s + 1) * rank], 0.0)
    high = part.astype(jnp.bfloat16)
    low = (part - high.astype(jnp.float32)).astype(jnp.bfloat16)
    out_ref[:, :cols] = rows
    out_ref[:, cols:] = jnp.concatenate(
        [high, low, jnp.zeros((row_count, LANES - 2 * rank), jnp.bfloat16)], axis=1
    )


def payload_body(x_ref, panel_ref, out_ref, *, seg_rows, rank):
    write_payload(out_ref, x_ref[...], panel_ref[...], seg_rows, rank)


def make_payload(x, panel, seg_rows, rank):
    rows, cols = x.shape
    out = jax.ShapeDtypeStruct((rows, cols + LANES), jnp.bfloat16)
    spec = kernel_call(
        functools.partial(payload_body, seg_rows=seg_rows, rank=rank),
        out,
        2 * rows * cols * panel.shape[0],
        4 * rows * cols,
        "payload",
    )
    return pl.pallas_call(in_specs=[vmem(), vmem()], out_specs=vmem(), **spec)(x, panel)


def chunk_copies(weight, targets, starts, depth, sems, base):
    rows = weight.shape[0]
    pieces = PIECES if rows % (PIECES * 16) == 0 else 1
    size = rows // pieces
    out = []
    for c, (target, start) in enumerate(zip(targets, starts)):
        for p in range(pieces):
            part = pl.ds(p * size, size)
            out.append(
                pltpu.make_async_copy(
                    weight.at[part, pl.ds(start, depth)],
                    target.at[part, :],
                    sems.at[(base + c) * PIECES + p],
                )
            )
    return out


def tile_of(size):
    for parts in (2, 1):
        if size % (parts * LANES) == 0:
            return size // parts
    return size


def stage_body(info_ref, *refs, kind, gate, slots, later, begin, finish, shape):
    row_count, depth, seg_rows, rank, features, segments, slot_at, live_at = shape
    count = len(slots)
    chunks, refs = refs[:count], refs[count:]
    weight_ref, refs = refs[0], refs[1:]
    if begin:
        held = None
    else:
        held, refs = refs[:count], refs[count:]
    if kind == "up":
        gain_ref, refs = refs[0], refs[1:]
    if finish == "act":
        panel_ref, refs = refs[0], refs[1:]
    if finish in ("next", "last"):
        own_ref, side_ref, refs = refs[0], refs[1], refs[2:]
    if not begin:
        total_in, refs = refs[0], refs[1:]
        if kind == "up":
            stat_in, refs = refs[0], refs[1:]
    ahead, refs = refs[: len(later)], refs[len(later) :]
    if finish:
        out_ref, refs = refs[0], refs[1:]
        total_ref, stat_ref = None, None
        if kind == "up":
            stat_ref, refs = refs[0], refs[1:]
    else:
        total_ref, refs = refs[0], refs[1:]
        if kind == "up":
            stat_ref, refs = refs[0], refs[1:]
    if begin:
        held, refs = refs[:count], refs[count:]
    sems = refs[0] if refs else None
    width = weight_ref.shape[0]
    tile = tile_of(width)
    active = info_ref[gate] == 1

    def start_of(slot):
        return pl.multiple_of(info_ref[slot_at + slot] * depth, LANES)

    @pl.when(active)
    def _():
        mine = []
        if begin:
            mine = chunk_copies(weight_ref, held, [start_of(s) for s in slots], depth, sems, 0)
            for copy in mine:
                copy.start()
        base = count if begin else 0
        coming = chunk_copies(weight_ref, ahead, [start_of(s) for s in later], depth, sems, base)
        for copy in coming:
            copy.start()
        lefts = []
        for c in range(count):
            if kind == "down":
                lefts.append(chunks[c][...])
                continue
            wide = chunks[c][:, :depth].astype(jnp.float32)
            lefts.append((wide * gain_ref[:, pl.ds(start_of(slots[c]), depth)]).astype(jnp.bfloat16))
            squares = jnp.sum(wide * wide, axis=1, keepdims=True)
            extra = chunks[c][:, depth:].astype(jnp.float32)
            low = extra[:, :rank] + extra[:, rank : 2 * rank]
            stat = jnp.concatenate(
                [low, jnp.broadcast_to(squares, (row_count, LANES - rank))], axis=1
            )
            if c == 0 and begin:
                stat_ref[...] = stat
            elif c == 0:
                stat_ref[...] = stat_in[...] + stat
            else:
                stat_ref[...] += stat
        if finish == "act":
            inverse = lax.rsqrt(stat_ref[:, rank : rank + 1] / features + EPSILON)
            low = (inverse * stat_ref[:, :rank]).astype(jnp.bfloat16)
            across = panel_ref.shape[0]
            tiled = jnp.concatenate([low] * segments, axis=1).astype(jnp.float32)
            row = lax.broadcasted_iota(jnp.int32, (row_count, across), 0)
            col = lax.broadcasted_iota(jnp.int32, (row_count, across), 1)
            keep = jnp.zeros((row_count, across), jnp.bool_)
            for s in range(segments):
                rows_in = jnp.logical_and(row >= s * seg_rows, row < (s + 1) * seg_rows)
                cols_in = jnp.logical_and(col >= s * rank, col < (s + 1) * rank)
                keep = jnp.logical_or(keep, jnp.logical_and(rows_in, cols_in))
            spread_low = jnp.where(keep, tiled, 0.0).astype(jnp.bfloat16)
        if finish in ("next", "last"):
            row = lax.broadcasted_iota(jnp.int32, (row_count, 1), 0)
            keep = jnp.zeros((row_count, 1), jnp.bool_)
            for s in range(segments):
                end = info_ref[live_at + s] + s * seg_rows
                keep = jnp.logical_or(keep, jnp.logical_and(row >= s * seg_rows, row < end))
        for copy in mine:
            copy.wait()

        def one_tile(j):
            part = pl.ds(pl.multiple_of(j * tile, tile), tile)
            value = None if begin else total_in[:, part]
            for c in range(count):
                term = lax.dot_general(
                    lefts[c],
                    held[c][part, :],
                    (((1,), (1,)), ((), ())),
                    preferred_element_type=jnp.float32,
                )
                value = term if value is None else value + term
            if finish == "act":
                adapted = jnp.dot(
                    spread_low, panel_ref[:, part], preferred_element_type=jnp.float32
                )
                value = inverse * value + adapted
                out_ref[:, part] = (value / (1.0 + jnp.exp(-value))).astype(jnp.bfloat16)
            elif finish:
                value = own_ref[:, part].astype(jnp.float32) + value
                out_ref[:, part] = jnp.where(keep, value, 0.0).astype(jnp.bfloat16)
            else:
                total_ref[:, part] = value

        pl.loop(0, width // tile)(one_tile)
        if finish == "next":
            write_payload(out_ref, out_ref[:, :width], side_ref[...], seg_rows, rank)
        for copy in coming:
            copy.wait()

    if finish == "last":

        @pl.when(jnp.logical_not(active))
        def _():
            out_ref[...] = side_ref[:, :width]


def stage_call(
    kind, info, gate, slots, later, chunks, weight, held, state, shape, name, gain=None, extras=(),
    finish=None,
):
    row_count, depth = shape[0], shape[1]
    width = weight.shape[0]
    begin = state is None
    operands = [info] + list(chunks) + [in_hbm(weight)]
    specs = [smem()] + [vmem()] * len(chunks) + [anywhere()]
    if not begin:
        operands += list(held)
    if kind == "up":
        operands.append(gain)
    operands += list(extras)
    aliases = {}
    outs = [jax.ShapeDtypeStruct((width, depth), jnp.bfloat16) for _ in later]
    if finish == "act":
        outs.append(jax.ShapeDtypeStruct((row_count, width), jnp.bfloat16))
    elif finish == "next":
        outs.append(jax.ShapeDtypeStruct((row_count, width + LANES), jnp.bfloat16))
    elif finish == "last":
        outs.append(jax.ShapeDtypeStruct((row_count, width), jnp.bfloat16))
    else:
        outs.append(jax.ShapeDtypeStruct((row_count, width), jnp.float32))
    if kind == "up":
        outs.append(jax.ShapeDtypeStruct((row_count, LANES), jnp.float32))
    if not begin:
        if not finish:
            aliases[len(operands)] = len(later)
        operands.append(state[0])
        if kind == "up":
            aliases[len(operands)] = len(later) + 1
            operands.append(state[1])
    specs += [vmem()] * (len(operands) - len(specs))
    scratch = []
    if begin:
        scratch += [pltpu.VMEM((width, depth), jnp.bfloat16) for _ in slots]
    moving = len(later) + (len(slots) if begin else 0)
    if moving:
        scratch.append(pltpu.SemaphoreType.DMA((moving * PIECES,)))
    spec = kernel_call(
        functools.partial(
            stage_body,
            kind=kind,
            gate=gate,
            slots=tuple(slots),
            later=tuple(later),
            begin=begin,
            finish=finish,
            shape=shape,
        ),
        tuple(outs),
        2 * row_count * width * depth * len(slots),
        2 * width * depth * (len(slots) + len(later)),
        name,
        aliases,
        scratch,
    )
    got = pl.pallas_call(in_specs=specs, out_specs=(vmem(),) * len(outs), **spec)(*operands)
    return list(got[: len(later)]), list(got[len(later) :])


def plan_of(rungs):
    order = sorted(range(1, rungs), key=lambda k: min(k, rungs - k))
    names = ["own", "x0"] + [f"z{k}" for k in order] + [f"f{k}" for k in order]
    if not order:
        return order, names, [["x0"]]
    groups = [[f"z{order[0]}", "x0"]]
    for a, b in zip(order, order[1:]):
        groups.append([f"f{a}", f"z{b}"])
    groups.append([f"f{order[-1]}"])
    return order, names, groups


def run_ladder(
    rows, ids, live, gain, up_weight, down_weight, shrink_weight, expand_weight, rails
):
    row_count, cols = rows.shape
    segments = ids.shape[0]
    seg_rows = row_count // segments
    rank = shrink_weight.shape[1] // cols
    units = up_weight.shape[0]
    features = gain.shape[0]
    me = lax.axis_index("tp")
    stage = lax.axis_index("pipe")
    size = lax.axis_size("tp")
    rungs = size // rails
    rung, rail = me // rails, me % rails
    order, names, groups = plan_of(rungs)

    def send(value, source, target, move):
        pairs = []
        for t in range(size):
            g, r = move(t // rails, t % rails)
            pairs.append((source * size + t, target * size + g % rungs * rails + r))
        return lax.ppermute(value, ("pipe", "tp"), pairs)

    def owner(step, on):
        return (rung - step + rungs) % rungs * rails + on

    owners = {"own": me, "x0": owner(0, 1 - rail)}
    for k in order:
        owners[f"z{k}"] = owner(k, rail)
        owners[f"f{k}"] = owner(k, 1 - rail)
    gates = [(stage == k).astype(jnp.int32) for k in range(2)]
    table = jnp.stack(gates + [owners[n].astype(jnp.int32) for n in names])
    info = jnp.concatenate([table, live, ids])
    slot_at, live_at = 2, 2 + len(names)
    id_at = live_at + segments
    slot = {n: i for i, n in enumerate(names)}

    gain_row = gain.reshape(1, features)
    (shrink_rows,), gain_mine = fetch_rows(
        info, gain_row, [shrink_weight], segments, id_at, slot_at, cols
    )
    reduce_panel = jnp.concatenate(
        [r.reshape(1, cols, rank).transpose(0, 2, 1) for r in shrink_rows]
    )
    reduce_panel = (
        (reduce_panel.astype(jnp.float32) * gain_mine[:, None, :])
        .astype(jnp.bfloat16)
        .reshape(segments * rank, cols)
    )
    swap = [(i, (i + size) % (2 * size)) for i in range(2 * size)]
    partner_panel = lax.ppermute(reduce_panel, ("pipe", "tp"), swap)
    first_panel = jnp.where(stage == 0, reduce_panel, partner_panel)
    carried = make_payload(rows, first_panel, seg_rows, rank)
    (expand_rows,), _ = fetch_rows(
        info, gain_row, [expand_weight], segments, id_at, slot_at, cols
    )
    expand_panel = jnp.concatenate(
        [r.reshape(1, units, rank).transpose(0, 2, 1) for r in expand_rows]
    ).reshape(segments * rank, units)

    def gather(value, worker):
        helper = 1 - worker
        got = {}
        for k in order:
            got[f"z{k}"] = send(value, helper, worker, lambda g, r, k=k: (g + k, r))
        got["x0"] = send(value, helper, worker, lambda g, r: (g, 1 - r))
        for k in order:
            got[f"f{k}"] = send(got[f"z{k}"], worker, worker, lambda g, r: (g, 1 - r))
        return got

    def multiply(kind, own, got, weight, gate, depth, phase, gain=None, extras=(), finish=None):
        shape = (row_count, depth, seg_rows, rank, features, segments, slot_at, live_at)
        held, state = None, None
        steps = [["own"]] + groups
        for i, group in enumerate(steps):
            later = [slot[n] for n in steps[i + 1]] if i + 1 < len(steps) else []
            last = not later
            held, state = stage_call(
                kind,
                info,
                gate,
                [slot[n] for n in group],
                later,
                [own if n == "own" else got[n] for n in group],
                weight,
                held,
                state,
                shape,
                phase + ("_own" if i == 0 else f"_{i - 1}"),
                gain=gain,
                extras=extras if last else (),
                finish=finish if last else None,
            )
        return state[0]

    for k in range(2):
        worker, helper = k, 1 - k
        own = carried
        if k:
            own = send(carried, helper, worker, lambda g, r: (g, r))
        got = gather(carried, worker)
        act = multiply(
            "up", own, got, up_weight, k, cols, f"{k}x", gain_row, (expand_panel,), "act"
        )
        handed = send(act, worker, helper, lambda g, r: (g, r))
        got = gather(handed, worker)
        side = partner_panel if k == 0 else carried
        carried = multiply(
            "down", act, got, down_weight, k, units, f"{k}a", None, (own, side),
            "next" if k == 0 else "last",
        )
    return carried


def per_device(
    hidden_entering,
    segment_adapter,
    segment_requests,
    section_norm_gain,
    up_matrix,
    down_matrix,
    adapter_reduce,
    adapter_expand,
):
    batch_list = hidden_entering.shape[0]
    row_count = hidden_entering.shape[1]
    col_count = hidden_entering.shape[2]
    size = lax.axis_size("tp")
    rails = 2
    fits = (
        lax.axis_size("pipe") == 2
        and batch_list == 1
        and size % rails == 0
        and size // rails <= 4
        and col_count % LANES == 0
        and up_matrix.shape[1] % LANES == 0
    )
    if fits:
        out = run_ladder(
            hidden_entering[0],
            segment_adapter[0],
            segment_requests[0],
            section_norm_gain[0],
            up_matrix[0],
            down_matrix[0],
            adapter_reduce[0],
            adapter_expand[0],
            rails,
        )
        return out.reshape(1, batch_list, row_count, col_count)
    collected = run_window(
        hidden_entering,
        segment_adapter,
        segment_requests,
        section_norm_gain[0],
        up_matrix[0],
        down_matrix[0],
        adapter_reduce[0],
        adapter_expand[0],
    )
    return collected.reshape(1, batch_list, row_count, col_count)


def solution(mesh):
    return jax.shard_map(
        per_device,
        mesh=mesh,
        in_specs=(
            P("rep", None, "tp"),
            P("rep", None),
            P("rep", None),
            P("pipe", None),
            P("pipe", "tp", None),
            P("pipe", "tp", None),
            P("pipe", None, "tp"),
            P("pipe", None, "tp"),
        ),
        out_specs=P("pipe", "rep", None, "tp"),
        check_vma=False,
    )
```
